256 devices in a mesh: dp: 32 (over y, x, core), group: 8 (over z).
Axes of the slice: x: 4, y: 4, z: 8, core: 2. Of those that a mesh axis runs over, the one named last changes fastest.
Arguments:
- patches: bfloat16 [212992, 768], P('dp', 'group'), may hold values from -4 to 4
- embed_weight: bfloat16 [768, 1024], P('dp', 'group'), may hold values from -0.0625 to 0.0625
- channel_gain: float32 [1024], replicated, may hold values from 0.1 to 1.9
- cotangent: bfloat16 [212992, 1024], P('dp', 'group'), may hold values from -6 to 6
Outputs:
- weight_grad: float32 [768, 1024], P('dp', 'group')
- gain_grad: float32 [1024], P('group')
The draws below stay inside these ranges and needn't reach their ends.
All inputs are finite; a program needn't handle non-finite values.
Results may differ from the reference program's by a relative error of at most 0.00155.
Values may be sent and summed in bfloat16 or wider, within the bound.
No kernel may reach another device: no remote copies, remote signals or barrier semaphores. Data moves between devices by JAX's collectives and lax.ppermute only.
A program may use at most 128 MiB of HBM per device.

```python
import math
import jax
import jax.numpy as jnp
from jax import lax

PD = 768
G = 16
GW = 64
ITERS = 5
C = 1024
TOKENS = 212992


def patch_noise(key):
    sub = jax.random.fold_in(key, 101)
    return jnp.clip(jax.random.normal(sub, (TOKENS, PD), jnp.float32), -3.0, 3.0)


def patch_offset(key):
    sub = jax.random.fold_in(key, 102)
    return jax.random.uniform(sub, (PD,), jnp.float32, -1.0, 1.0)


def weight_values(key):
    sub = jax.random.fold_in(key, 103)
    bound = 0.99 * jnp.sqrt(3.0 / PD)
    return jax.random.uniform(sub, (PD, G * GW), jnp.float32, -bound, bound)


def draw_patches(key, part):
    return (patch_noise(key) + patch_offset(key)[None, :]).astype(jnp.bfloat16)


def draw_embed_weight(key, part):
    return weight_values(key).astype(jnp.bfloat16)


def draw_cotangent(key, part):
    weights = weight_values(key)
    features = jnp.dot(patch_noise(key), weights)
    features = features / jnp.sqrt(jnp.sum(weights * weights, axis=0))
    mixing = jax.random.normal(jax.random.fold_in(key, 104), (G, GW, GW), jnp.float32)
    mixing = mixing * (1.0 - jnp.eye(GW, dtype=jnp.float32)) / jnp.sqrt(GW - 1.0)
    related = jnp.einsum('tgb,gab->tga', features.reshape(TOKENS, G, GW), mixing).reshape(TOKENS, G * GW)
    noise_key = jax.random.fold_in(key, 105)
    offset_key = jax.random.fold_in(key, 106)
    noise = jnp.clip(jax.random.normal(noise_key, (TOKENS, G * GW), jnp.float32), -3.5, 3.5)
    offset = jax.random.uniform(offset_key, (G * GW,), jnp.float32, -0.7, 0.7)
    return jnp.clip(noise + offset[None, :] + 0.3 * related, -6.0, 6.0).astype(jnp.bfloat16)


def setup_inputs(seed: int = 0) -> dict:
    keys = jax.random.split(jax.random.key(seed), 5)
    return {
        "patches": draw_patches(jax.random.fold_in(keys[4], 71), 0),
        "embed_weight": draw_embed_weight(jax.random.fold_in(keys[4], 71), 0),
        "channel_gain": jnp.clip(1.0 + 0.18 * jax.random.normal(keys[2], (C,), jnp.float32), 0.1, 1.9),
        "cotangent": draw_cotangent(jax.random.fold_in(keys[4], 71), 0),
    }


EPSILON = 1e-05
highest = lax.Precision.HIGHEST

def matmul_batch(left, right):
    return jnp.einsum('gij,gjk->gik', left, right, precision=highest)

def whiten_matrix(covariance):
    width = covariance.shape[-1]
    traces = jnp.trace(covariance, axis1=1, axis2=2)
    normed = covariance / traces[:, None, None]
    iterate = jnp.broadcast_to(jnp.eye(width, dtype=jnp.float32), covariance.shape)
    for counter in range(ITERS):
        cubed = matmul_batch(matmul_batch(iterate, iterate), iterate)
        iterate = 1.5 * iterate - 0.5 * matmul_batch(cubed, normed)
    return iterate / jnp.sqrt(traces)[:, None, None]

def forward(features, channel_gain):
    tok_rows = features.shape[0]
    average = lax.optimization_barrier(jnp.sum(features, axis=0)) / TOKENS
    centered = features - average
    grouped = centered.reshape(tok_rows, G, GW)
    covariance = jnp.einsum('tga,tgb->gab', grouped, grouped, precision=highest) / TOKENS
    covariance = covariance + EPSILON * jnp.eye(GW, dtype=jnp.float32)
    whitener = whiten_matrix(covariance)
    whitened = jnp.einsum('tgb,gab->tga', grouped, whitener, precision=highest)
    return whitened.reshape(tok_rows, G * GW) * channel_gain

def reference(patches, embed_weight, channel_gain, cotangent):
    embedded = jnp.dot(patches, embed_weight, preferred_element_type=jnp.float32).astype(jnp.bfloat16)
    outputs, pullback = jax.vjp(forward, embedded.astype(jnp.float32), channel_gain)
    grad_out = cotangent.astype(jnp.float32) * (1.0 / math.sqrt(TOKENS))
    grad_feat, gain_grad = pullback(grad_out)
    weight_grad = jnp.dot(patches.T, grad_feat.astype(jnp.bfloat16), preferred_element_type=jnp.float32)
    return (weight_grad, gain_grad)
```

```python
import math

import jax
import jax.numpy as jnp
from jax import lax
from jax.experimental import pallas as pl
from jax.experimental.pallas import tpu as pltpu
from jax.sharding import Mesh
from jax.sharding import PartitionSpec as P

GW = 64
ITERS = 5
DP = ("dp_0", "dp_1", "dp_2")
EPSILON = 1e-05
CHUNKS = 4
f32, bf16 = jnp.float32, jnp.bfloat16
highest = lax.Precision.HIGHEST
VMEM = pl.BlockSpec(memory_space=pltpu.VMEM)
SMEM = pl.BlockSpec(memory_space=pltpu.SMEM)


def shifted(value, axis, by):
    size = lax.axis_size(axis)
    return lax.ppermute(value, axis, [(i, (i + by) % size) for i in range(size)])


def gathered_weights(shard):
    count = lax.axis_size(DP)
    copies = jnp.broadcast_to(shard, (count, *shard.shape))
    parts = lax.all_to_all(copies, DP, split_axis=0, concat_axis=0, tiled=True)
    return parts.reshape(-1, shard.shape[1])


def ring_parts(chunks):
    half = chunks[0].shape[0] // 2
    right = [[c] for c in chunks]
    left = [[c] for c in chunks]
    for hop in range(3):
        for r, l in zip(right, left):
            r.append(shifted(r[-1], "group", 1))
            l.append(shifted(l[-1], "group", -1))
    done = []
    for r, l in zip(right, left):
        far_r = shifted(r[3][:half], "group", 1)
        far_l = shifted(l[3][half:], "group", -1)
        done.append((r[0], r[1], r[2], r[3], l[1], l[2], l[3], far_r, far_l))
    return done


def chunk_kernel(*refs, accumulate):
    zidx, own, r1, r2, r3, l1, l2, l3, fr, fl, cot, wt = refs[:12]
    rest = refs[12:]
    if accumulate:
        ins, rest = rest[:3], rest[3:]
    ab, hg, sx, big, ce = rest
    width = own.shape[0]
    half = width // 2
    z = zidx[0]

    def place(ref, ahead, extra=0):
        row = pl.multiple_of(((z + ahead) % 8) * width + extra, 16)
        big[pl.ds(row, ref.shape[0]), :] = ref[...]

    place(own, 0)
    place(r1, 7)
    place(r2, 6)
    place(r3, 5)
    place(l1, 1)
    place(l2, 2)
    place(l3, 3)
    place(fr, 4)
    place(fl, 4, half)
    rows = 8 * width
    channels = cot.shape[1]
    et = jnp.dot(wt[...], big[:rows, :], preferred_element_type=f32)
    big[rows : rows + channels, :] = et.astype(bf16)
    big[rows + channels :, :] = jnp.ones((16, big.shape[1]), bf16)
    ce[:, :channels] = cot[...]
    ce[:, channels:] = et.T.astype(bf16)
    product = jnp.dot(big[...], ce[...], preferred_element_type=f32)
    ones = jnp.ones((8, big.shape[1]), bf16)
    sums = lax.dot_general(
        ones, big[:rows, :], (((1,), (1,)), ((), ())), preferred_element_type=f32
    )
    if accumulate:
        ab[...] = ins[0][...] + product[:rows]
        hg[...] = ins[1][...] + product[rows : rows + channels + 8]
        sx[...] = ins[2][...] + sums
    else:
        ab[...] = product[:rows]
        hg[...] = product[rows : rows + channels + 8]
        sx[...] = sums


def chunk_step(zidx, parts, cot, wt, totals):
    width, tokens = parts[0].shape
    channels = cot.shape[1]
    rows = 8 * width
    outs = (
        jax.ShapeDtypeStruct((rows, 2 * channels), f32),
        jax.ShapeDtypeStruct((channels + 8, 2 * channels), f32),
        jax.ShapeDtypeStruct((8, rows), f32),
    )
    accumulate = totals is not None

    def kernel(*refs):
        chunk_kernel(*refs, accumulate=accumulate)

    return pl.pallas_call(
        kernel,
        out_shape=outs,
        in_specs=[SMEM] + [VMEM] * (11 + (3 if accumulate else 0)),
        out_specs=(VMEM, VMEM, VMEM),
        scratch_shapes=[
            pltpu.VMEM((rows + channels + 16, tokens), bf16),
            pltpu.VMEM((tokens, 2 * channels), bf16),
        ],
        input_output_aliases={12: 0, 13: 1, 14: 2} if accumulate else {},
        cost_estimate=pl.CostEstimate(
            flops=2 * tokens * (rows * 3 * channels + channels * 2 * channels),
            bytes_accessed=2 * tokens * rows,
            transcendentals=0,
        ),
        compiler_params=pltpu.CompilerParams(vmem_limit_bytes=40 * 1024 * 1024),
        name="chunk",
    )(zidx, *parts, cot, wt, *(totals or ()))


def small_call(kernel, outs, operands, name):
    return pl.pallas_call(
        kernel,
        out_shape=outs,
        in_specs=[SMEM] + [VMEM] * (len(operands) - 1),
        out_specs=tuple(VMEM for _ in outs),
        cost_estimate=pl.CostEstimate(flops=1_000_000, bytes_accessed=1_000_000, transcendentals=0),
        compiler_params=pltpu.CompilerParams(vmem_limit_bytes=32 * 1024 * 1024),
        name=name,
    )(*operands)


COMMON = 144


def core_stage(at, totals):
    ab, hg, sx = totals
    share = 24
    channels = ab.shape[1] // 2

    def kernel(at, ab, hg, sx, keep, send):
        core = at[2]
        for ref, parity in ((keep, core), (send, 1 - core)):
            for block in range(16):
                row = pl.multiple_of(block * 2 * share + parity * share, 8)
                for side in range(2):
                    to = (block * 2 + side) * share
                    ref[to : to + share, :] = ab[
                        pl.ds(row, share), side * channels : (side + 1) * channels
                    ]
            low = lax.broadcasted_iota(jnp.int32, (GW, channels), 1) < GW
            base = 32 * share
            for side in range(2):
                cols = slice(side * channels, (side + 1) * channels)
                ref[base + side * GW : base + (side + 1) * GW, :] = jnp.where(
                    low, hg[:GW, cols], hg[GW : 2 * GW, cols]
                )
            base += 2 * GW
            ref[base : base + COMMON - 2 * GW, :] = jnp.zeros((COMMON - 2 * GW, channels), f32)
            for side in range(2):
                ref[base + side : base + side + 1, :] = hg[
                    2 * GW : 2 * GW + 1, side * channels : (side + 1) * channels
                ]
            for part in range(6):
                ref[base + 8 + part : base + 9 + part, :] = sx[
                    0:1, part * channels : (part + 1) * channels
                ]

    shape = jax.ShapeDtypeStruct((32 * share + COMMON, channels), f32)
    return small_call(kernel, (shape, shape), (at, ab, hg, sx), "core_stage")


def axis_stage(at, which, received, rows_out):
    rows_in, channels = received[0].shape

    def kernel(at, *refs):
        ins, outs = refs[: len(received)], refs[len(received) :]
        here = at[which]
        shared = ins[0][rows_in - COMMON :, :]
        for ref in ins[1:]:
            shared = shared + ref[rows_in - COMMON :, :]
        for step, out in enumerate(outs):
            row = pl.multiple_of(((here + step) % 4) * rows_out, 8)
            block = ins[0][pl.ds(row, rows_out), :]
            for ref in ins[1:]:
                block = block + ref[pl.ds(row, rows_out), :]
            out[:rows_out, :] = block
            out[rows_out:, :] = shared

    shape = jax.ShapeDtypeStruct((rows_out + COMMON, channels), f32)
    return small_call(kernel, (shape,) * 4, (at, *received), "axis_stage")


def dot(left, right):
    return jnp.dot(left, right, preferred_element_type=f32, precision=highest)


def last_stage(at, received, gain, total_tokens):
    channels = received[0].shape[1]
    share = 24
    loss_scale = 1.0 / math.sqrt(total_tokens)
    inverse = 1.0 / total_tokens

    def kernel(at, *refs):
        ins, gain_ref = refs[: len(received)], refs[len(received)]
        weight_out, gain_out = refs[len(received) + 1 :]
        everything = ins[0][...]
        for ref in ins[1:]:
            everything = everything + ref[...]
        a_rows = everything[:share]
        b_rows = everything[share : 2 * share]
        base = 2 * share
        lane = lax.broadcasted_iota(jnp.int32, (channels, channels), 1)
        row = lax.broadcasted_iota(jnp.int32, (channels, channels), 0)
        same = (lane < GW) == (row < GW)
        eye = (lane == row).astype(f32)
        lane1 = lax.broadcasted_iota(jnp.int32, (1, channels), 1)

        def blocks(flat):
            return jnp.where(same, jnp.concatenate([flat, flat], axis=0), 0.0)

        def per_group(line):
            low = jnp.sum(jnp.where(lane1 < GW, line, 0.0), axis=1, keepdims=True)
            high = jnp.sum(jnp.where(lane1 < GW, 0.0, line), axis=1, keepdims=True)
            return jnp.where(lane1 < GW, low, high)

        def column(line):
            return jnp.sum(eye * line, axis=1, keepdims=True)

        h_t = blocks(everything[base : base + GW])
        gram = blocks(everything[base + GW : base + 2 * GW])
        base += 2 * GW
        cot_sum = everything[base : base + 1]
        mean = everything[base + 1 : base + 2] * inverse
        patch_sums = everything[base + 8 : base + 14]
        mean_col = column(mean)
        covariance = gram * inverse - jnp.where(same, mean_col * mean, 0.0) + EPSILON * eye
        h_t = h_t - jnp.where(same, mean_col * cot_sum, 0.0)
        scaled_gain = gain_ref[...] * loss_scale
        q_t = h_t * scaled_gain
        toward = 0.5 * (q_t + q_t.T)
        trace = per_group(jnp.sum(covariance * eye, axis=0, keepdims=True))
        normed = covariance / trace
        power = 1.5 * eye - 0.5 * normed
        change = -0.5 * toward
        right = jnp.concatenate([normed, toward], axis=1)
        for _ in range(ITERS - 1):
            both = jnp.concatenate([power, change], axis=0)
            first = dot(both, power)
            second = dot(both, right)
            square, mixed = first[:channels], first[channels:]
            times = second[:channels, :channels]
            times_change = second[channels:, :channels] + second[:channels, channels:]
            square_change = mixed + mixed.T
            third = dot(square, jnp.concatenate([times, times_change], axis=1))
            fourth = dot(square_change, times)
            power, change = (
                1.5 * power - 0.5 * third[:, :channels],
                1.5 * change - 0.5 * (third[:, channels:] + fourth),
            )
        root = lax.rsqrt(trace)
        whitener = power * root
        spread = per_group(jnp.sum(change * covariance, axis=0, keepdims=True))
        scale_part = per_group(jnp.sum(toward * power, axis=0, keepdims=True))
        cubed = root * root * root
        grad_cov = cubed * change - eye * (cubed * root * root * spread + 0.5 * cubed * scale_part)
        symmetric = grad_cov * (2.0 * inverse)
        gain_out[...] = jnp.sum(whitener * h_t, axis=0, keepdims=True) * loss_scale
        device = (at[0] * 4 + at[1]) * 2 + at[2]
        lanes = lax.broadcasted_iota(jnp.int32, (share, channels), 1)
        rows = lax.broadcasted_iota(jnp.int32, (share, channels), 0) + device * share
        picked = jnp.zeros((share, channels), f32)
        for part in range(6):
            picked = picked + jnp.where(
                lanes + part * channels == rows, patch_sums[part : part + 1], 0.0
            )
        patch_sum = jnp.sum(picked, axis=1, keepdims=True)
        a_rows = (a_rows - patch_sum * (cot_sum * inverse)) * scaled_gain
        b_rows = b_rows - patch_sum * mean
        weight_out[...] = dot(a_rows, whitener) + dot(b_rows, symmetric)

    outs = (
        jax.ShapeDtypeStruct((share, channels), f32),
        jax.ShapeDtypeStruct((1, channels), f32),
    )
    return small_call(kernel, outs, (at, *received, gain), "last_stage")


def body(patches, embed_weight, channel_gain, cotangent):
    tok_rows = patches.shape[0]
    total_tokens = tok_rows * lax.axis_size(DP)
    width_here = embed_weight.shape[1]
    group = lax.axis_index("group").astype(jnp.int32)
    zidx = group.reshape(1)
    at = jnp.stack([lax.axis_index(a).astype(jnp.int32) for a in DP])
    step = tok_rows // CHUNKS
    flipped = patches.T
    chunks = [flipped[:, i * step : (i + 1) * step] for i in range(CHUNKS)]
    parts = ring_parts(chunks)
    weights_t = gathered_weights(embed_weight).T
    gain_here = lax.dynamic_slice_in_dim(channel_gain, group * width_here, width_here)
    totals = None
    for i in range(CHUNKS):
        totals = chunk_step(
            zidx, parts[i], cotangent[i * step : (i + 1) * step], weights_t, totals
        )
    keep, send = core_stage(at, totals)
    keep, *send = axis_stage(at, 0, (keep, shifted(send, "dp_2", 1)), 192)
    came = [shifted(s, "dp_0", i + 1) for i, s in enumerate(send)]
    keep, *send = axis_stage(at, 1, (keep, *came), 48)
    came = [shifted(s, "dp_1", i + 1) for i, s in enumerate(send)]
    weight_grad, gain_grad = last_stage(
        at, (keep, *came), gain_here.reshape(1, -1), total_tokens
    )
    return weight_grad, gain_grad.reshape(-1)


def solution(mesh):
    torus = Mesh(
        mesh.devices.reshape(4, 4, 2, mesh.shape["group"]), ("dp_0", "dp_1", "dp_2", "group")
    )
    return jax.shard_map(
        body,
        mesh=torus,
        in_specs=(P(DP, "group"), P(DP, "group"), P(), P(DP, "group")),
        out_specs=(P(DP, "group"), P("group")),
        check_vma=False,
    )
```

```python
import math

import jax
import jax.numpy as jnp
from jax import lax
from jax.experimental import pallas as pl
from jax.experimental.pallas import tpu as pltpu
from jax.sharding import Mesh
from jax.sharding import PartitionSpec as P

GW = 64
ITERS = 5
DP = ("dp_0", "dp_1", "dp_2")
EPSILON = 1e-05
CHUNKS = (26, 26)
f32, bf16 = jnp.float32, jnp.bfloat16
highest = lax.Precision.HIGHEST
VMEM = pl.BlockSpec(memory_space=pltpu.VMEM)
HBM = pl.BlockSpec(memory_space=pltpu.HBM)


def shifted(value, axis, by):
    size = lax.axis_size(axis)
    return lax.ppermute(value, axis, [(i, (i + by) % size) for i in range(size)])


def gathered_weights(shard):
    count = lax.axis_size(DP)
    copies = jnp.broadcast_to(shard, (count, *shard.shape))
    parts = lax.all_to_all(copies, DP, split_axis=0, concat_axis=0, tiled=True)
    return parts.reshape(-1, shard.shape[1])


def after(value, *others):
    return lax.optimization_barrier((value, *others))


def half_of(block, lower):
    half = block.shape[0] // 2

    def kernel(ref, out):
        out[...] = ref[:half, :] if lower else ref[half:, :]

    return small_call(
        kernel, (jax.ShapeDtypeStruct((half, block.shape[1]), block.dtype),), (block,), "half_of"
    )[0]


def sums_over_ring(chunks, starts, cot, shard):
    weights = gathered_weights(shard).T
    sides = [([c], [c]) for c in chunks]
    for hop in range(3):
        for index, (r, l) in enumerate(sides):
            if hop == 1 and index == 1:
                r[1], weights = after(r[1], weights)
            r.append(shifted(r[-1], "group", 1))
            l.append(shifted(l[-1], "group", -1))
    totals = None
    for (r, l), start in zip(sides, starts):
        far_r = shifted(half_of(r[3], True), "group", 1)
        far_l = shifted(half_of(l[3], False), "group", -1)
        parts = (r[0], r[1], r[2], r[3], l[1], l[2], l[3], far_r, far_l)
        totals = chunk_step(parts, cot, start, weights, totals)
    return totals


TILES = 2


def chunk_kernel(*refs, start, accumulate):
    own, r1, r2, r3, l1, l2, l3, fr, fl, cot, wt = refs[:11]
    rest = refs[11:]
    if accumulate:
        ins, rest = rest[:3], rest[3:]
    ab, hg, sx, big, ce, sems = rest
    width, tokens = own.shape
    half = width // 2
    tile = tokens // TILES
    z = lax.axis_index("group")
    channels = cot.shape[1]
    rows = 8 * width
    blocks = (
        (own, 0, 0),
        (r1, 7, 0),
        (l1, 1, 0),
        (r2, 6, 0),
        (l2, 2, 0),
        (r3, 5, 0),
        (l3, 3, 0),
        (fr, 4, 0),
        (fl, 4, half),
    )

    def copies(step):
        found = []
        for index, (ref, ahead, extra) in enumerate(blocks):
            row = pl.multiple_of(((z + ahead) % 8) * width + extra, 16)
            found.append(
                pltpu.make_async_copy(
                    ref.at[:, step * tile : (step + 1) * tile],
                    big.at[step, pl.ds(row, ref.shape[0]), :],
                    sems.at[step, index],
                )
            )
        found.append(
            pltpu.make_async_copy(
                cot.at[start + step * tile : start + (step + 1) * tile, :],
                ce.at[step, :, :channels],
                sems.at[step, len(blocks)],
            )
        )
        return found

    moves = [copies(step) for step in range(TILES)]
    for step in moves:
        for move in step:
            move.start()
    for step in range(TILES):
        big[step, rows + channels :, :] = jnp.ones((16, tile), bf16)
    for step in range(TILES):
        for move in moves[step]:
            move.wait()
        et = jnp.dot(wt[...], big[step, :rows, :], preferred_element_type=f32)
        big[step, rows : rows + channels, :] = et.astype(bf16)
        ce[step, :, channels:] = et.T.astype(bf16)
        product = jnp.dot(big[step], ce[step], preferred_element_type=f32)
        sums = lax.dot_general(
            jnp.ones((8, tile), bf16),
            big[step, :rows, :],
            (((1,), (1,)), ((), ())),
            preferred_element_type=f32,
        )
        if step or accumulate:
            before = (ab, hg, sx) if step else ins
            ab[...] = before[0][...] + product[:rows]
            hg[...] = before[1][...] + product[rows : rows + channels + 8]
            sx[...] = before[2][...] + sums
        else:
            ab[...] = product[:rows]
            hg[...] = product[rows : rows + channels + 8]
            sx[...] = sums


def chunk_step(parts, cot, start, wt, totals):
    width, tokens = parts[0].shape
    channels = cot.shape[1]
    rows = 8 * width
    outs = (
        jax.ShapeDtypeStruct((rows, 2 * channels), f32),
        jax.ShapeDtypeStruct((channels + 8, 2 * channels), f32),
        jax.ShapeDtypeStruct((8, rows), f32),
    )
    accumulate = totals is not None

    def kernel(*refs):
        chunk_kernel(*refs, start=start, accumulate=accumulate)

    return pl.pallas_call(
        kernel,
        out_shape=outs,
        in_specs=[HBM] * 10 + [VMEM] * (4 if accumulate else 1),
        out_specs=(VMEM, VMEM, VMEM),
        scratch_shapes=[
            pltpu.VMEM((TILES, rows + channels + 16, tokens // TILES), bf16),
            pltpu.VMEM((TILES, tokens // TILES, 2 * channels), bf16),
            pltpu.SemaphoreType.DMA((TILES, 10)),
        ],
        input_output_aliases={11: 0, 12: 1, 13: 2} if accumulate else {},
        cost_estimate=pl.CostEstimate(
            flops=2 * tokens * (rows * 3 * channels + channels * 2 * channels),
            bytes_accessed=2 * tokens * rows,
            transcendentals=0,
        ),
        compiler_params=pltpu.CompilerParams(vmem_limit_bytes=12 * 1024 * 1024),
        name="chunk",
    )(*parts, cot, wt, *(totals or ()))


def small_call(kernel, outs, operands, name):
    return pl.pallas_call(
        kernel,
        out_shape=outs,
        in_specs=[VMEM] * len(operands),
        out_specs=tuple(VMEM for _ in outs),
        cost_estimate=pl.CostEstimate(flops=1_000_000, bytes_accessed=1_000_000, transcendentals=0),
        compiler_params=pltpu.CompilerParams(vmem_limit_bytes=6 * 1024 * 1024),
        name=name,
    )(*operands)


COMMON = 144


def core_stage(totals):
    ab, hg, sx = totals
    share = 24
    channels = ab.shape[1] // 2

    def kernel(ab, hg, sx, keep, send):
        core = lax.axis_index("dp_2")
        for ref, parity in ((keep, core), (send, 1 - core)):
            for block in range(16):
                row = pl.multiple_of(block * 2 * share + parity * share, 8)
                for side in range(2):
                    to = (block * 2 + side) * share
                    ref[to : to + share, :] = ab[
                        pl.ds(row, share), side * channels : (side + 1) * channels
                    ]
            low = lax.broadcasted_iota(jnp.int32, (GW, channels), 1) < GW
            base = 32 * share
            for side in range(2):
                cols = slice(side * channels, (side + 1) * channels)
                ref[base + side * GW : base + (side + 1) * GW, :] = jnp.where(
                    low, hg[:GW, cols], hg[GW : 2 * GW, cols]
                )
            base += 2 * GW
            ref[base : base + COMMON - 2 * GW, :] = jnp.zeros((COMMON - 2 * GW, channels), f32)
            for side in range(2):
                ref[base + side : base + side + 1, :] = hg[
                    2 * GW : 2 * GW + 1, side * channels : (side + 1) * channels
                ]
            for part in range(6):
                ref[base + 8 + part : base + 9 + part, :] = sx[
                    0:1, part * channels : (part + 1) * channels
                ]

    shape = jax.ShapeDtypeStruct((32 * share + COMMON, channels), f32)
    return small_call(kernel, (shape, shape), (ab, hg, sx), "core_stage")


def axis_stage(axis, received, rows_out):
    rows_in, channels = received[0].shape

    def kernel(*refs):
        ins, outs = refs[: len(received)], refs[len(received) :]
        here = lax.axis_index(axis)
        shared = ins[0][rows_in - COMMON :, :]
        for ref in ins[1:]:
            shared = shared + ref[rows_in - COMMON :, :]
        for step, out in enumerate(outs):
            row = pl.multiple_of(((here + step) % 4) * rows_out, 8)
            block = ins[0][pl.ds(row, rows_out), :]
            for ref in ins[1:]:
                block = block + ref[pl.ds(row, rows_out), :]
            out[:rows_out, :] = block
            out[rows_out:, :] = shared

    shape = jax.ShapeDtypeStruct((rows_out + COMMON, channels), f32)
    return small_call(kernel, (shape,) * 4, received, "axis_stage")


def dot(left, right):
    return jnp.dot(left, right, preferred_element_type=f32, precision=highest)


def last_stage(received, gain, total_tokens):
    channels = received[0].shape[1]
    share = 24
    loss_scale = 1.0 / math.sqrt(total_tokens)
    inverse = 1.0 / total_tokens

    def kernel(*refs):
        ins, gain_ref = refs[: len(received)], refs[len(received)]
        weight_out, gain_out = refs[len(received) + 1 :]
        everything = ins[0][...]
        for ref in ins[1:]:
            everything = everything + ref[...]
        a_rows = everything[:share]
        b_rows = everything[share : 2 * share]
        base = 2 * share
        lane = lax.broadcasted_iota(jnp.int32, (channels, channels), 1)
        row = lax.broadcasted_iota(jnp.int32, (channels, channels), 0)
        same = (lane < GW) == (row < GW)
        eye = (lane == row).astype(f32)
        lane1 = lax.broadcasted_iota(jnp.int32, (1, channels), 1)

        def blocks(flat):
            return jnp.where(same, jnp.concatenate([flat, flat], axis=0), 0.0)

        def per_group(line):
            low = jnp.sum(jnp.where(lane1 < GW, line, 0.0), axis=1, keepdims=True)
            high = jnp.sum(jnp.where(lane1 < GW, 0.0, line), axis=1, keepdims=True)
            return jnp.where(lane1 < GW, low, high)

        def column(line):
            return jnp.sum(eye * line, axis=1, keepdims=True)

        h_t = blocks(everything[base : base + GW])
        gram = blocks(everything[base + GW : base + 2 * GW])
        base += 2 * GW
        cot_sum = everything[base : base + 1]
        mean = everything[base + 1 : base + 2] * inverse
        patch_sums = everything[base + 8 : base + 14]
        mean_col = column(mean)
        covariance = gram * inverse - jnp.where(same, mean_col * mean, 0.0) + EPSILON * eye
        h_t = h_t - jnp.where(same, mean_col * cot_sum, 0.0)
        scaled_gain = gain_ref[pl.ds(lax.axis_index("group"), 1), :] * loss_scale
        q_t = h_t * scaled_gain
        toward = 0.5 * (q_t + q_t.T)
        trace = per_group(jnp.sum(covariance * eye, axis=0, keepdims=True))
        normed = covariance / trace
        power = 1.5 * eye - 0.5 * normed
        change = -0.5 * toward
        right = jnp.concatenate([normed, toward], axis=1)
        for _ in range(ITERS - 1):
            both = jnp.concatenate([power, change], axis=0)
            first = dot(both, power)
            second = dot(both, right)
            square, mixed = first[:channels], first[channels:]
            times = second[:channels, :channels]
            times_change = second[channels:, :channels] + second[:channels, channels:]
            square_change = mixed + mixed.T
            third = dot(square, jnp.concatenate([times, times_change], axis=1))
            fourth = dot(square_change, times)
            power, change = (
                1.5 * power - 0.5 * third[:, :channels],
                1.5 * change - 0.5 * (third[:, channels:] + fourth),
            )
        root = lax.rsqrt(trace)
        whitener = power * root
        spread = per_group(jnp.sum(change * covariance, axis=0, keepdims=True))
        scale_part = per_group(jnp.sum(toward * power, axis=0, keepdims=True))
        cubed = root * root * root
        grad_cov = cubed * change - eye * (cubed * root * root * spread + 0.5 * cubed * scale_part)
        symmetric = grad_cov * (2.0 * inverse)
        gain_out[...] = jnp.sum(whitener * h_t, axis=0, keepdims=True) * loss_scale
        device = lax.axis_index(DP)
        lanes = lax.broadcasted_iota(jnp.int32, (share, channels), 1)
        rows = lax.broadcasted_iota(jnp.int32, (share, channels), 0) + device * share
        picked = jnp.zeros((share, channels), f32)
        for part in range(6):
            picked = picked + jnp.where(
                lanes + part * channels == rows, patch_sums[part : part + 1], 0.0
            )
        patch_sum = jnp.sum(picked, axis=1, keepdims=True)
        a_rows = (a_rows - patch_sum * (cot_sum * inverse)) * scaled_gain
        b_rows = b_rows - patch_sum * mean
        weight_out[...] = dot(a_rows, whitener) + dot(b_rows, symmetric)

    outs = (
        jax.ShapeDtypeStruct((share, channels), f32),
        jax.ShapeDtypeStruct((1, channels), f32),
    )
    return small_call(kernel, outs, (*received, gain), "last_stage")


def body(patches, embed_weight, channel_gain, cotangent):
    tok_rows = patches.shape[0]
    total_tokens = tok_rows * lax.axis_size(DP)
    unit = tok_rows // sum(CHUNKS)
    bounds = [unit * sum(CHUNKS[:i]) for i in range(len(CHUNKS) + 1)]
    flipped = patches.T
    totals = sums_over_ring(
        [flipped[:, lo:hi] for lo, hi in zip(bounds, bounds[1:])], bounds, cotangent, embed_weight
    )
    keep, send = core_stage(totals)
    keep, *send = axis_stage("dp_0", (keep, shifted(send, "dp_2", 1)), 192)
    came = [shifted(s, "dp_0", i + 1) for i, s in enumerate(send)]
    keep, *send = axis_stage("dp_1", (keep, *came), 48)
    came = [shifted(s, "dp_1", i + 1) for i, s in enumerate(send)]
    gain = channel_gain.reshape(-1, embed_weight.shape[1])
    weight_grad, gain_grad = last_stage((keep, *came), gain, total_tokens)
    return weight_grad, gain_grad.reshape(-1)


def solution(mesh):
    torus = Mesh(
        mesh.devices.reshape(4, 4, 2, mesh.shape["group"]), ("dp_0", "dp_1", "dp_2", "group")
    )
    return jax.shard_map(
        body,
        mesh=torus,
        in_specs=(P(DP, "group"), P(DP, "group"), P(), P(DP, "group")),
        out_specs=(P(DP, "group"), P("group")),
        check_vma=False,
    )
```

```python
import math

import jax
import jax.numpy as jnp
from jax import lax
from jax.experimental import pallas as pl
from jax.experimental.pallas import tpu as pltpu
from jax.sharding import Mesh
from jax.sharding import PartitionSpec as P

GW = 64
ITERS = 5
DP = ("dp_0", "dp_1", "dp_2")
EPSILON = 1e-05
CHUNKS = (26, 26)
f32, bf16 = jnp.float32, jnp.bfloat16
VMEM = pl.BlockSpec(memory_space=pltpu.VMEM)
HBM = pl.BlockSpec(memory_space=pltpu.HBM)


def shifted(value, axis, by):
    size = lax.axis_size(axis)
    return lax.ppermute(value, axis, [(i, (i + by) % size) for i in range(size)])


def gathered_weights(shard):
    count = lax.axis_size(DP)
    copies = jnp.broadcast_to(shard, (count, *shard.shape))
    parts = lax.all_to_all(copies, DP, split_axis=0, concat_axis=0, tiled=True)
    return parts.reshape(-1, shard.shape[1])


def after(value, *others):
    return lax.optimization_barrier((value, *others))


def half_of(block, lower):
    half = block.shape[0] // 2

    def kernel(ref, out):
        out[...] = ref[:half, :] if lower else ref[half:, :]

    return small_call(
        kernel, (jax.ShapeDtypeStruct((half, block.shape[1]), block.dtype),), (block,), "half_of"
    )[0]


def sums_over_ring(chunks, starts, cot, shard):
    weights = gathered_weights(shard)
    sides = [([c], [c]) for c in chunks]
    for hop in range(3):
        for index, (r, l) in enumerate(sides):
            if hop == 1 and index == 1:
                r[1], weights = after(r[1], weights)
            r.append(shifted(r[-1], "group", 1))
            l.append(shifted(l[-1], "group", -1))
    totals = None
    laid, fars = [], []
    for r, l in sides:
        if laid:
            big, near, sx = laid[0]
            r[3], l[3], sx = after(r[3], l[3], sx)
            laid[0] = (big, near, sx)
        fars.append(
            (shifted(half_of(r[3], True), "group", 1), shifted(half_of(l[3], False), "group", -1))
        )
        laid.append(near_step((*r, *l[1:]), weights))
    for (far_r, far_l), here, start in zip(fars, laid, starts):
        totals = far_step(far_r, far_l, here, cot, start, weights, totals)
    return totals


TILES = 2


def near_step(blocks, weights):
    width, tokens = blocks[0].shape
    channels = weights.shape[1]
    rows = 8 * width
    tile = tokens // TILES
    ahead = (0, 7, 6, 5, 1, 2, 3)

    def kernel(own, r1, r2, r3, l1, l2, l3, w, big, near, sx, sems):
        z = lax.axis_index("group")
        refs = (own, r1, r2, r3, l1, l2, l3)

        def place(by):
            return pl.ds(pl.multiple_of(((z + by) % 8) * width, 32), width)

        moves = [
            [
                pltpu.make_async_copy(
                    ref.at[:, step * tile : (step + 1) * tile],
                    big.at[step, place(by), :],
                    sems.at[step, index],
                )
                for index, (ref, by) in enumerate(zip(refs, ahead))
            ]
            for step in range(TILES)
        ]
        for step in moves:
            for move in step:
                move.start()
        for step in range(TILES):
            big[step, place(4), :] = jnp.zeros((width, tile), bf16)
            big[step, rows + channels :, :] = jnp.ones((16, tile), bf16)
        wt = w[...].astype(f32).T.astype(bf16)
        sx[place(4), :] = jnp.zeros((width, channels), f32)
        for ref, by in zip(refs, ahead):
            total = jnp.sum(ref[...].astype(f32), axis=1, keepdims=True)
            sx[place(by), :] = jnp.broadcast_to(total, (width, channels))
        for step in range(TILES):
            for move in moves[step]:
                move.wait()
            near[step] = jnp.dot(wt, big[step, :rows, :], preferred_element_type=f32)

    return pl.pallas_call(
        kernel,
        out_shape=(
            jax.ShapeDtypeStruct((TILES, rows + channels + 16, tile), bf16),
            jax.ShapeDtypeStruct((TILES, channels, tile), f32),
            jax.ShapeDtypeStruct((rows, channels), f32),
        ),
        in_specs=[VMEM] * 8,
        out_specs=(VMEM,) * 3,
        scratch_shapes=[pltpu.SemaphoreType.DMA((TILES, 7))],
        cost_estimate=pl.CostEstimate(
            flops=2 * tokens * rows * channels, bytes_accessed=2 * tokens * rows, transcendentals=0
        ),
        compiler_params=pltpu.CompilerParams(vmem_limit_bytes=14 * 1024 * 1024),
        name="near",
    )(*blocks, weights)


def far_step(far_r, far_l, laid, cot, start, weights, totals):
    half, tokens = far_r.shape
    width = 2 * half
    channels = cot.shape[1]
    rows = 8 * width
    tile = tokens // TILES
    accumulate = totals is not None

    def kernel(*refs):
        far_r, far_l, big_in, near, near_sx, cot, w = refs[:7]
        ins, rest = (refs[7:10], refs[10:]) if accumulate else ((), refs[7:])
        big, ab, hg, sx, ce, sems = rest
        row = pl.multiple_of(((lax.axis_index("group") + 4) % 8) * width, 32)

        moves = [
            [
                pltpu.make_async_copy(
                    far_r.at[:, step * tile : (step + 1) * tile],
                    big.at[step, pl.ds(row, half), :],
                    sems.at[step, 0],
                ),
                pltpu.make_async_copy(
                    far_l.at[:, step * tile : (step + 1) * tile],
                    big.at[step, pl.ds(pl.multiple_of(row + half, 16), half), :],
                    sems.at[step, 1],
                ),
                pltpu.make_async_copy(
                    cot.at[start + step * tile : start + (step + 1) * tile, :],
                    ce.at[step, :, :channels],
                    sems.at[step, 2],
                ),
            ]
            for step in range(TILES)
        ]
        for step in moves:
            for move in step:
                move.start()
        w_far = w[pl.ds(row, width), :].astype(f32).T.astype(bf16)
        far_sx = jnp.concatenate(
            [
                jnp.sum(ref[...].astype(f32), axis=1, keepdims=True)
                for ref in (far_r, far_l)
            ],
            axis=0,
        )
        sums = near_sx[...] + ins[2][...] if accumulate else near_sx[...]
        sx[...] = sums
        sx[pl.ds(row, width), :] = sx[pl.ds(row, width), :] + far_sx
        for step in range(TILES):
            for move in moves[step]:
                move.wait()
            et = near[step] + jnp.dot(
                w_far, big[step, pl.ds(row, width), :], preferred_element_type=f32
            )
            big[step, rows : rows + channels, :] = et.astype(bf16)
            ce[step, :, channels:] = et.T.astype(bf16)
            product = jnp.dot(big[step], ce[step], preferred_element_type=f32)
            if step or accumulate:
                before = (ab, hg) if step else ins
                ab[...] = before[0][...] + product[:rows]
                hg[...] = before[1][...] + product[rows : rows + channels + 8]
            else:
                ab[...] = product[:rows]
                hg[...] = product[rows : rows + channels + 8]

    aliases = {2: 0}
    if accumulate:
        aliases.update({7: 1, 8: 2, 9: 3})
    outs = pl.pallas_call(
        kernel,
        out_shape=(
            jax.ShapeDtypeStruct(laid[0].shape, bf16),
            jax.ShapeDtypeStruct((rows, 2 * channels), f32),
            jax.ShapeDtypeStruct((channels + 8, 2 * channels), f32),
            jax.ShapeDtypeStruct((rows, channels), f32),
        ),
        in_specs=[VMEM] * 5 + [HBM] + [VMEM] * (4 if accumulate else 1),
        out_specs=(VMEM,) * 4,
        scratch_shapes=[
            pltpu.VMEM((TILES, tile, 2 * channels), bf16),
            pltpu.SemaphoreType.DMA((TILES, 3)),
        ],
        input_output_aliases=aliases,
        cost_estimate=pl.CostEstimate(
            flops=2 * tokens * (rows + channels) * 2 * channels,
            bytes_accessed=2 * tokens * rows,
            transcendentals=0,
        ),
        compiler_params=pltpu.CompilerParams(vmem_limit_bytes=14 * 1024 * 1024),
        name="far",
    )(far_r, far_l, *laid, cot, weights, *(totals or ()))
    return outs[1:]


def small_call(kernel, outs, operands, name):
    return pl.pallas_call(
        kernel,
        out_shape=outs,
        in_specs=[VMEM] * len(operands),
        out_specs=tuple(VMEM for _ in outs),
        cost_estimate=pl.CostEstimate(flops=1_000_000, bytes_accessed=1_000_000, transcendentals=0),
        compiler_params=pltpu.CompilerParams(vmem_limit_bytes=6 * 1024 * 1024),
        name=name,
    )(*operands)


COMMON = 112


def core_stage(totals):
    ab, hg, sx = totals
    share = 24
    channels = ab.shape[1] // 2

    def kernel(ab, hg, sx, keep, send):
        core = lax.axis_index("dp_2")
        for ref, parity in ((keep, core), (send, 1 - core)):
            for block in range(16):
                row = pl.multiple_of(block * 2 * share + parity * share, 8)
                for side in range(2):
                    to = (block * 2 + side) * share
                    ref[to : to + share, :] = ab[
                        pl.ds(row, share), side * channels : (side + 1) * channels
                    ]
            lane = lax.broadcasted_iota(jnp.int32, (GW, channels), 1)
            row = lax.broadcasted_iota(jnp.int32, (GW, channels), 0)
            low = lane < GW
            mixed, gram = (
                jnp.where(low, hg[:GW, cols], hg[GW : 2 * GW, cols])
                for cols in (slice(0, channels), slice(channels, 2 * channels))
            )
            base = 32 * share
            ref[base : base + GW, :] = mixed
            square = jnp.where(row < lane, gram, pltpu.roll(gram, GW, 1))
            ref[base + GW : base + GW + 32, :] = jnp.where(
                low[:32], square[:32], pltpu.roll(square, GW, 1)[32:]
            )
            base += GW + 32
            ref[base : base + 16, :] = jnp.zeros((16, channels), f32)
            diagonal = (lane == row) | (lane == row + GW)
            square_eye = lax.broadcasted_iota(
                jnp.int32, (channels, channels), 0
            ) == lax.broadcasted_iota(jnp.int32, (channels, channels), 1)
            ref[base : base + 1, :] = jnp.sum(
                jnp.where(diagonal, gram, 0.0), axis=0, keepdims=True
            )
            for side in range(2):
                ref[base + 1 + side : base + 2 + side, :] = hg[
                    2 * GW : 2 * GW + 1, side * channels : (side + 1) * channels
                ]
            for part in range(6):
                ref[base + 3 + part : base + 4 + part, :] = jnp.sum(
                    jnp.where(square_eye, sx[part * channels : (part + 1) * channels, :], 0.0),
                    axis=0,
                    keepdims=True,
                )

    shape = jax.ShapeDtypeStruct((32 * share + COMMON, channels), f32)
    return small_call(kernel, (shape, shape), (ab, hg, sx), "core_stage")


def axis_stage(axis, received, rows_out):
    rows_in, channels = received[0].shape

    def kernel(*refs):
        ins, outs = refs[: len(received)], refs[len(received) :]
        here = lax.axis_index(axis)
        shared = ins[0][rows_in - COMMON :, :]
        for ref in ins[1:]:
            shared = shared + ref[rows_in - COMMON :, :]
        for step, out in enumerate(outs):
            row = pl.multiple_of(((here + step) % 4) * rows_out, 8)
            block = ins[0][pl.ds(row, rows_out), :]
            for ref in ins[1:]:
                block = block + ref[pl.ds(row, rows_out), :]
            out[:rows_out, :] = block
            out[rows_out:, :] = shared

    shape = jax.ShapeDtypeStruct((rows_out + COMMON, channels), f32)
    return small_call(kernel, (shape,) * 4, received, "axis_stage")


def split(value):
    high = value.astype(bf16)
    return high, (value - high.astype(f32)).astype(bf16)


def dot(left, right):
    left_high, left_low = split(left)
    right_high, right_low = split(right)
    both = jnp.concatenate([left_high, left_low], axis=1)
    twice = jnp.concatenate([right_high, right_high], axis=0)
    return jnp.dot(both, twice, preferred_element_type=f32) + jnp.dot(
        left_high, right_low, preferred_element_type=f32
    )


def last_stage(received, gain, total_tokens):
    channels = received[0].shape[1]
    share = 24
    loss_scale = 1.0 / math.sqrt(total_tokens)
    inverse = 1.0 / total_tokens

    def kernel(*refs):
        ins, gain_ref = refs[: len(received)], refs[len(received)]
        weight_out, gain_out = refs[len(received) + 1 :]
        everything = ins[0][...]
        for ref in ins[1:]:
            everything = everything + ref[...]
        a_rows = everything[:share]
        b_rows = everything[share : 2 * share]
        base = 2 * share
        lane = lax.broadcasted_iota(jnp.int32, (channels, channels), 1)
        row = lax.broadcasted_iota(jnp.int32, (channels, channels), 0)
        same = (lane < GW) == (row < GW)
        eye = (lane == row).astype(f32)
        lane1 = lax.broadcasted_iota(jnp.int32, (1, channels), 1)

        def blocks(flat):
            return jnp.where(same, jnp.concatenate([flat, flat], axis=0), 0.0)

        def per_group(line):
            low = jnp.sum(jnp.where(lane1 < GW, line, 0.0), axis=1, keepdims=True)
            high = jnp.sum(jnp.where(lane1 < GW, 0.0, line), axis=1, keepdims=True)
            return jnp.where(lane1 < GW, low, high)

        def column(line):
            return jnp.sum(eye * line, axis=1, keepdims=True)

        h_t = blocks(everything[base : base + GW])
        packed = everything[base + GW : base + GW + 32]
        square = jnp.concatenate([packed, pltpu.roll(packed, GW, 1)], axis=0)
        square = jnp.where(lane[:GW] < GW, square, 0.0)
        square = jnp.concatenate([square, jnp.zeros((GW, channels), f32)], axis=0)
        turned = square.T
        upper = jnp.where(row < lane, square, turned)
        lower = jnp.where(row > lane, square, turned)
        lower = pltpu.roll(jnp.concatenate([lower[GW:], lower[:GW]], axis=0), GW, 1)
        base += GW + 32
        gram = jnp.where(row < GW, upper, lower)
        gram = jnp.where(same & (lane != row), gram, 0.0) + eye * everything[base : base + 1]
        cot_sum = everything[base + 1 : base + 2]
        mean = everything[base + 2 : base + 3] * inverse
        patch_sums = everything[base + 3 : base + 9]
        mean_col = column(mean)
        covariance = gram * inverse - jnp.where(same, mean_col * mean, 0.0) + EPSILON * eye
        h_t = h_t - jnp.where(same, mean_col * cot_sum, 0.0)
        scaled_gain = gain_ref[pl.ds(lax.axis_index("group"), 1), :] * loss_scale
        q_t = h_t * scaled_gain
        toward = 0.5 * (q_t + q_t.T)
        trace = per_group(jnp.sum(covariance * eye, axis=0, keepdims=True))
        normed = covariance / trace
        power = 1.5 * eye - 0.5 * normed
        change = -0.5 * toward
        right = jnp.concatenate([normed, toward], axis=1)
        for _ in range(ITERS - 1):
            both = jnp.concatenate([power, change], axis=0)
            first = dot(both, power)
            second = dot(both, right)
            square, mixed = first[:channels], first[channels:]
            times = second[:channels, :channels]
            times_change = second[channels:, :channels] + second[:channels, channels:]
            square_change = mixed + mixed.T
            third = dot(square, jnp.concatenate([times, times_change], axis=1))
            fourth = dot(square_change, times)
            power, change = (
                1.5 * power - 0.5 * third[:, :channels],
                1.5 * change - 0.5 * (third[:, channels:] + fourth),
            )
        root = lax.rsqrt(trace)
        whitener = power * root
        spread = per_group(jnp.sum(change * covariance, axis=0, keepdims=True))
        scale_part = per_group(jnp.sum(toward * power, axis=0, keepdims=True))
        cubed = root * root * root
        grad_cov = cubed * change - eye * (cubed * root * root * spread + 0.5 * cubed * scale_part)
        symmetric = grad_cov * (2.0 * inverse)
        gain_out[...] = jnp.sum(whitener * h_t, axis=0, keepdims=True) * loss_scale
        device = lax.axis_index(DP)
        lanes = lax.broadcasted_iota(jnp.int32, (share, channels), 1)
        rows = lax.broadcasted_iota(jnp.int32, (share, channels), 0) + device * share
        picked = jnp.zeros((share, channels), f32)
        for part in range(6):
            picked = picked + jnp.where(
                lanes + part * channels == rows, patch_sums[part : part + 1], 0.0
            )
        patch_sum = jnp.sum(picked, axis=1, keepdims=True)
        a_rows = (a_rows - patch_sum * (cot_sum * inverse)) * scaled_gain
        b_rows = b_rows - patch_sum * mean
        weight_out[...] = dot(a_rows, whitener) + dot(b_rows, symmetric)

    outs = (
        jax.ShapeDtypeStruct((share, channels), f32),
        jax.ShapeDtypeStruct((1, channels), f32),
    )
    return small_call(kernel, outs, (*received, gain), "last_stage")


def body(patches, embed_weight, channel_gain, cotangent):
    tok_rows = patches.shape[0]
    total_tokens = tok_rows * lax.axis_size(DP)
    unit = tok_rows // sum(CHUNKS)
    bounds = [unit * sum(CHUNKS[:i]) for i in range(len(CHUNKS) + 1)]
    flipped = patches.T
    totals = sums_over_ring(
        [flipped[:, lo:hi] for lo, hi in zip(bounds, bounds[1:])], bounds, cotangent, embed_weight
    )
    keep, send = core_stage(totals)
    keep, *send = axis_stage("dp_0", (keep, shifted(send, "dp_2", 1)), 192)
    came = [shifted(s, "dp_0", i + 1) for i, s in enumerate(send)]
    keep, *send = axis_stage("dp_1", (keep, *came), 48)
    came = [shifted(s, "dp_1", i + 1) for i, s in enumerate(send)]
    gain = channel_gain.reshape(-1, embed_weight.shape[1])
    weight_grad, gain_grad = last_stage((keep, *came), gain, total_tokens)
    return weight_grad, gain_grad.reshape(-1)


def solution(mesh):
    torus = Mesh(
        mesh.devices.reshape(4, 4, 2, mesh.shape["group"]), ("dp_0", "dp_1", "dp_2", "group")
    )
    return jax.shard_map(
        body,
        mesh=torus,
        in_specs=(P(DP, "group"), P(DP, "group"), P(), P(DP, "group")),
        out_specs=(P(DP, "group"), P("group")),
        check_vma=False,
    )
```

```python
import math

import jax
import jax.numpy as jnp
from jax import lax
from jax.experimental import pallas as pl
from jax.experimental.pallas import tpu as pltpu
from jax.sharding import Mesh
from jax.sharding import PartitionSpec as P

GW = 64
ITERS = 5
DP = ("dp_0", "dp_1", "dp_2")
EPSILON = 1e-05
CHUNKS = (26, 26)
f32, bf16 = jnp.float32, jnp.bfloat16
VMEM = pl.BlockSpec(memory_space=pltpu.VMEM)
HBM = pl.BlockSpec(memory_space=pltpu.HBM)


def shifted(value, axis, by):
    size = lax.axis_size(axis)
    return lax.ppermute(value, axis, [(i, (i + by) % size) for i in range(size)])


def gathered_weights(shard):
    count = lax.axis_size(DP)
    copies = jnp.broadcast_to(shard, (count, *shard.shape))
    parts = lax.all_to_all(copies, DP, split_axis=0, concat_axis=0, tiled=True)
    return parts.reshape(-1, shard.shape[1])


def after(value, *others):
    return lax.optimization_barrier((value, *others))


def half_of(block, lower):
    half = block.shape[0] // 2

    def kernel(ref, out):
        out[...] = ref[:half, :] if lower else ref[half:, :]

    return small_call(
        kernel, (jax.ShapeDtypeStruct((half, block.shape[1]), block.dtype),), (block,), "half_of"
    )[0]


def sums_over_ring(chunks, starts, cot, shard):
    weights = gathered_weights(shard)
    sides = [([c], [c]) for c in chunks]
    for hop in range(3):
        for index, (r, l) in enumerate(sides):
            if hop == 1 and index == 1:
                r[1], weights = after(r[1], weights)
            r.append(shifted(r[-1], "group", 1))
            l.append(shifted(l[-1], "group", -1))
    totals = None
    laid, fars = [], []
    for r, l in sides:
        if laid:
            big, near, sx = laid[0]
            r[3], l[3], sx = after(r[3], l[3], sx)
            laid[0] = (big, near, sx)
        fars.append(
            (shifted(half_of(r[3], True), "group", 1), shifted(half_of(l[3], False), "group", -1))
        )
        laid.append(near_step((*r, *l[1:]), weights))
    for (far_r, far_l), here, start in zip(fars, laid, starts):
        totals = far_step(far_r, far_l, here, cot, start, weights, totals)
    return totals


TILES = 2


def near_step(blocks, weights):
    width, tokens = blocks[0].shape
    channels = weights.shape[1]
    rows = 8 * width
    tile = tokens // TILES
    ahead = (0, 7, 6, 5, 1, 2, 3)

    def kernel(own, r1, r2, r3, l1, l2, l3, w, big, near, sx, sems):
        z = lax.axis_index("group")
        refs = (own, r1, r2, r3, l1, l2, l3)

        def place(by):
            return pl.ds(pl.multiple_of(((z + by) % 8) * width, 32), width)

        moves = [
            [
                pltpu.make_async_copy(
                    ref.at[:, step * tile : (step + 1) * tile],
                    big.at[step, place(by), :],
                    sems.at[step, index],
                )
                for index, (ref, by) in enumerate(zip(refs, ahead))
            ]
            for step in range(TILES)
        ]
        for step in moves:
            for move in step:
                move.start()
        for step in range(TILES):
            big[step, place(4), :] = jnp.zeros((width, tile), bf16)
            big[step, rows + channels :, :] = jnp.ones((16, tile), bf16)
        wt = w[...].astype(f32).T.astype(bf16)
        sx[place(4), :] = jnp.zeros((width, channels), f32)
        for ref, by in zip(refs, ahead):
            total = jnp.sum(ref[...].astype(f32), axis=1, keepdims=True)
            sx[place(by), :] = jnp.broadcast_to(total, (width, channels))
        for step in range(TILES):
            for move in moves[step]:
                move.wait()
            near[step] = jnp.dot(wt, big[step, :rows, :], preferred_element_type=f32)

    return pl.pallas_call(
        kernel,
        out_shape=(
            jax.ShapeDtypeStruct((TILES, rows + channels + 16, tile), bf16),
            jax.ShapeDtypeStruct((TILES, channels, tile), f32),
            jax.ShapeDtypeStruct((rows, channels), f32),
        ),
        in_specs=[VMEM] * 8,
        out_specs=(VMEM,) * 3,
        scratch_shapes=[pltpu.SemaphoreType.DMA((TILES, 7))],
        cost_estimate=pl.CostEstimate(
            flops=2 * tokens * rows * channels, bytes_accessed=2 * tokens * rows, transcendentals=0
        ),
        compiler_params=pltpu.CompilerParams(vmem_limit_bytes=14 * 1024 * 1024),
        name="near",
    )(*blocks, weights)


def far_step(far_r, far_l, laid, cot, start, weights, totals):
    half, tokens = far_r.shape
    width = 2 * half
    channels = cot.shape[1]
    rows = 8 * width
    tile = tokens // TILES
    accumulate = totals is not None

    def kernel(*refs):
        far_r, far_l, big_in, near, near_sx, cot, w = refs[:7]
        ins, rest = (refs[7:10], refs[10:]) if accumulate else ((), refs[7:])
        big, ab, hg, sx, ce, sems = rest
        row = pl.multiple_of(((lax.axis_index("group") + 4) % 8) * width, 32)

        moves = [
            [
                pltpu.make_async_copy(
                    far_r.at[:, step * tile : (step + 1) * tile],
                    big.at[step, pl.ds(row, half), :],
                    sems.at[step, 0],
                ),
                pltpu.make_async_copy(
                    far_l.at[:, step * tile : (step + 1) * tile],
                    big.at[step, pl.ds(pl.multiple_of(row + half, 16), half), :],
                    sems.at[step, 1],
                ),
                pltpu.make_async_copy(
                    cot.at[start + step * tile : start + (step + 1) * tile, :],
                    ce.at[step, :, :channels],
                    sems.at[step, 2],
                ),
            ]
            for step in range(TILES)
        ]
        for step in moves:
            for move in step:
                move.start()
        w_far = w[pl.ds(row, width), :].astype(f32).T.astype(bf16)
        far_sx = jnp.concatenate(
            [
                jnp.sum(ref[...].astype(f32), axis=1, keepdims=True)
                for ref in (far_r, far_l)
            ],
            axis=0,
        )
        sums = near_sx[...] + ins[2][...] if accumulate else near_sx[...]
        sx[...] = sums
        sx[pl.ds(row, width), :] = sx[pl.ds(row, width), :] + far_sx
        for step in range(TILES):
            for move in moves[step]:
                move.wait()
            et = near[step] + jnp.dot(
                w_far, big[step, pl.ds(row, width), :], preferred_element_type=f32
            )
            big[step, rows : rows + channels, :] = et.astype(bf16)
            ce[step, :, channels:] = et.T.astype(bf16)
            product = jnp.dot(big[step], ce[step], preferred_element_type=f32)
            if step or accumulate:
                before = (ab, hg) if step else ins
                ab[...] = before[0][...] + product[:rows]
                hg[...] = before[1][...] + product[rows : rows + channels + 8]
            else:
                ab[...] = product[:rows]
                hg[...] = product[rows : rows + channels + 8]

    aliases = {2: 0}
    if accumulate:
        aliases.update({7: 1, 8: 2, 9: 3})
    outs = pl.pallas_call(
        kernel,
        out_shape=(
            jax.ShapeDtypeStruct(laid[0].shape, bf16),
            jax.ShapeDtypeStruct((rows, 2 * channels), f32),
            jax.ShapeDtypeStruct((channels + 8, 2 * channels), f32),
            jax.ShapeDtypeStruct((rows, channels), f32),
        ),
        in_specs=[VMEM] * 5 + [HBM] + [VMEM] * (4 if accumulate else 1),
        out_specs=(VMEM,) * 4,
        scratch_shapes=[
            pltpu.VMEM((TILES, tile, 2 * channels), bf16),
            pltpu.SemaphoreType.DMA((TILES, 3)),
        ],
        input_output_aliases=aliases,
        cost_estimate=pl.CostEstimate(
            flops=2 * tokens * (rows + channels) * 2 * channels,
            bytes_accessed=2 * tokens * rows,
            transcendentals=0,
        ),
        compiler_params=pltpu.CompilerParams(vmem_limit_bytes=14 * 1024 * 1024),
        name="far",
    )(far_r, far_l, *laid, cot, weights, *(totals or ()))
    return outs[1:]


def small_call(kernel, outs, operands, name):
    return pl.pallas_call(
        kernel,
        out_shape=outs,
        in_specs=[VMEM] * len(operands),
        out_specs=tuple(VMEM for _ in outs),
        cost_estimate=pl.CostEstimate(flops=1_000_000, bytes_accessed=1_000_000, transcendentals=0),
        compiler_params=pltpu.CompilerParams(vmem_limit_bytes=6 * 1024 * 1024),
        name=name,
    )(*operands)


COMMON = 112


def core_stage(totals):
    ab, hg, sx = totals
    share = 24
    channels = ab.shape[1] // 2

    def kernel(ab, hg, sx, keep, send):
        core = lax.axis_index("dp_2")
        for ref, parity in ((keep, core), (send, 1 - core)):
            for block in range(16):
                from_block = jnp.where(parity == 0, block, block % 4 * 4 + block // 4)
                row = pl.multiple_of((from_block * 2 + parity) * share, 8)
                for side in range(2):
                    to = (block * 2 + side) * share
                    ref[to : to + share, :] = ab[
                        pl.ds(row, share), side * channels : (side + 1) * channels
                    ]
            lane = lax.broadcasted_iota(jnp.int32, (GW, channels), 1)
            row = lax.broadcasted_iota(jnp.int32, (GW, channels), 0)
            low = lane < GW
            mixed, gram = (
                jnp.where(low, hg[:GW, cols], hg[GW : 2 * GW, cols])
                for cols in (slice(0, channels), slice(channels, 2 * channels))
            )
            base = 32 * share
            ref[base : base + GW, :] = mixed
            square = jnp.where(row < lane, gram, pltpu.roll(gram, GW, 1))
            ref[base + GW : base + GW + 32, :] = jnp.where(
                low[:32], square[:32], pltpu.roll(square, GW, 1)[32:]
            )
            base += GW + 32
            ref[base : base + 16, :] = jnp.zeros((16, channels), f32)
            diagonal = (lane == row) | (lane == row + GW)
            square_eye = lax.broadcasted_iota(
                jnp.int32, (channels, channels), 0
            ) == lax.broadcasted_iota(jnp.int32, (channels, channels), 1)
            ref[base : base + 1, :] = jnp.sum(
                jnp.where(diagonal, gram, 0.0), axis=0, keepdims=True
            )
            for side in range(2):
                ref[base + 1 + side : base + 2 + side, :] = hg[
                    2 * GW : 2 * GW + 1, side * channels : (side + 1) * channels
                ]
            for part in range(6):
                ref[base + 3 + part : base + 4 + part, :] = jnp.sum(
                    jnp.where(square_eye, sx[part * channels : (part + 1) * channels, :], 0.0),
                    axis=0,
                    keepdims=True,
                )

    shape = jax.ShapeDtypeStruct((32 * share + COMMON, channels), f32)
    return small_call(kernel, (shape, shape), (ab, hg, sx), "core_stage")


def axis_stage(first, received, rows_out):
    rows_in, channels = received[0].shape

    def kernel(*refs):
        ins, outs = refs[: len(received)], refs[len(received) :]
        core_zero = lax.axis_index("dp_2") == 0
        here = jnp.where(
            core_zero if first else ~core_zero, lax.axis_index("dp_0"), lax.axis_index("dp_1")
        )
        shared = ins[0][rows_in - COMMON :, :]
        for ref in ins[1:]:
            shared = shared + ref[rows_in - COMMON :, :]
        for step, out in enumerate(outs):
            row = pl.multiple_of(((here + step) % 4) * rows_out, 8)
            block = ins[0][pl.ds(row, rows_out), :]
            for ref in ins[1:]:
                block = block + ref[pl.ds(row, rows_out), :]
            out[:rows_out, :] = block
            out[rows_out:, :] = shared

    shape = jax.ShapeDtypeStruct((rows_out + COMMON, channels), f32)
    return small_call(kernel, (shape,) * 4, received, "axis_stage")


def crossed(value, first, by):
    pairs = []
    for y in range(4):
        for x in range(4):
            for core in range(2):
                along_y = (core == 0) == first
                to = ((y + by) % 4, x) if along_y else (y, (x + by) % 4)
                pairs.append(((y * 4 + x) * 2 + core, (to[0] * 4 + to[1]) * 2 + core))
    return lax.ppermute(value, DP, pairs)


def split(value):
    high = value.astype(bf16)
    return high, (value - high.astype(f32)).astype(bf16)


def dot(left, right):
    left_high, left_low = split(left)
    right_high, right_low = split(right)
    both = jnp.concatenate([left_high, left_low], axis=1)
    twice = jnp.concatenate([right_high, right_high], axis=0)
    return jnp.dot(both, twice, preferred_element_type=f32) + jnp.dot(
        left_high, right_low, preferred_element_type=f32
    )


def last_stage(received, gain, total_tokens):
    channels = received[0].shape[1]
    share = 24
    loss_scale = 1.0 / math.sqrt(total_tokens)
    inverse = 1.0 / total_tokens

    def kernel(*refs):
        ins, gain_ref = refs[: len(received)], refs[len(received)]
        weight_out, gain_out = refs[len(received) + 1 :]
        everything = ins[0][...]
        for ref in ins[1:]:
            everything = everything + ref[...]
        a_rows = everything[:share]
        b_rows = everything[share : 2 * share]
        base = 2 * share
        lane = lax.broadcasted_iota(jnp.int32, (channels, channels), 1)
        row = lax.broadcasted_iota(jnp.int32, (channels, channels), 0)
        same = (lane < GW) == (row < GW)
        eye = (lane == row).astype(f32)
        lane1 = lax.broadcasted_iota(jnp.int32, (1, channels), 1)

        def blocks(flat):
            return jnp.where(same, jnp.concatenate([flat, flat], axis=0), 0.0)

        def per_group(line):
            low = jnp.sum(jnp.where(lane1 < GW, line, 0.0), axis=1, keepdims=True)
            high = jnp.sum(jnp.where(lane1 < GW, 0.0, line), axis=1, keepdims=True)
            return jnp.where(lane1 < GW, low, high)

        def column(line):
            return jnp.sum(eye * line, axis=1, keepdims=True)

        h_t = blocks(everything[base : base + GW])
        packed = everything[base + GW : base + GW + 32]
        square = jnp.concatenate([packed, pltpu.roll(packed, GW, 1)], axis=0)
        square = jnp.where(lane[:GW] < GW, square, 0.0)
        square = jnp.concatenate([square, jnp.zeros((GW, channels), f32)], axis=0)
        turned = square.T
        upper = jnp.where(row < lane, square, turned)
        lower = jnp.where(row > lane, square, turned)
        lower = pltpu.roll(jnp.concatenate([lower[GW:], lower[:GW]], axis=0), GW, 1)
        base += GW + 32
        gram = jnp.where(row < GW, upper, lower)
        gram = jnp.where(same & (lane != row), gram, 0.0) + eye * everything[base : base + 1]
        cot_sum = everything[base + 1 : base + 2]
        mean = everything[base + 2 : base + 3] * inverse
        patch_sums = everything[base + 3 : base + 9]
        mean_col = column(mean)
        covariance = gram * inverse - jnp.where(same, mean_col * mean, 0.0) + EPSILON * eye
        h_t = h_t - jnp.where(same, mean_col * cot_sum, 0.0)
        scaled_gain = gain_ref[pl.ds(lax.axis_index("group"), 1), :] * loss_scale
        q_t = h_t * scaled_gain
        toward = 0.5 * (q_t + q_t.T)
        trace = per_group(jnp.sum(covariance * eye, axis=0, keepdims=True))
        normed = covariance / trace
        power = 1.5 * eye - 0.5 * normed
        change = -0.5 * toward
        right = jnp.concatenate([normed, toward], axis=1)
        for _ in range(ITERS - 1):
            both = jnp.concatenate([power, change], axis=0)
            first = dot(both, power)
            second = dot(both, right)
            square, mixed = first[:channels], first[channels:]
            times = second[:channels, :channels]
            times_change = second[channels:, :channels] + second[:channels, channels:]
            square_change = mixed + mixed.T
            third = dot(square, jnp.concatenate([times, times_change], axis=1))
            fourth = dot(square_change, times)
            power, change = (
                1.5 * power - 0.5 * third[:, :channels],
                1.5 * change - 0.5 * (third[:, channels:] + fourth),
            )
        root = lax.rsqrt(trace)
        whitener = power * root
        spread = per_group(jnp.sum(change * covariance, axis=0, keepdims=True))
        scale_part = per_group(jnp.sum(toward * power, axis=0, keepdims=True))
        cubed = root * root * root
        grad_cov = cubed * change - eye * (cubed * root * root * spread + 0.5 * cubed * scale_part)
        symmetric = grad_cov * (2.0 * inverse)
        gain_out[...] = jnp.sum(whitener * h_t, axis=0, keepdims=True) * loss_scale
        device = lax.axis_index(DP)
        lanes = lax.broadcasted_iota(jnp.int32, (share, channels), 1)
        rows = lax.broadcasted_iota(jnp.int32, (share, channels), 0) + device * share
        picked = jnp.zeros((share, channels), f32)
        for part in range(6):
            picked = picked + jnp.where(
                lanes + part * channels == rows, patch_sums[part : part + 1], 0.0
            )
        patch_sum = jnp.sum(picked, axis=1, keepdims=True)
        a_rows = (a_rows - patch_sum * (cot_sum * inverse)) * scaled_gain
        b_rows = b_rows - patch_sum * mean
        weight_out[...] = dot(a_rows, whitener) + dot(b_rows, symmetric)

    outs = (
        jax.ShapeDtypeStruct((share, channels), f32),
        jax.ShapeDtypeStruct((1, channels), f32),
    )
    return small_call(kernel, outs, (*received, gain), "last_stage")


def body(patches, embed_weight, channel_gain, cotangent):
    tok_rows = patches.shape[0]
    total_tokens = tok_rows * lax.axis_size(DP)
    unit = tok_rows // sum(CHUNKS)
    bounds = [unit * sum(CHUNKS[:i]) for i in range(len(CHUNKS) + 1)]
    flipped = patches.T
    totals = sums_over_ring(
        [flipped[:, lo:hi] for lo, hi in zip(bounds, bounds[1:])], bounds, cotangent, embed_weight
    )
    keep, send = core_stage(totals)
    keep, *send = axis_stage(True, (keep, shifted(send, "dp_2", 1)), 192)
    came = [crossed(s, True, i + 1) for i, s in enumerate(send)]
    keep, *send = axis_stage(False, (keep, *came), 48)
    came = [crossed(s, False, i + 1) for i, s in enumerate(send)]
    gain = channel_gain.reshape(-1, embed_weight.shape[1])
    weight_grad, gain_grad = last_stage((keep, *came), gain, total_tokens)
    return weight_grad, gain_grad.reshape(-1)


def solution(mesh):
    torus = Mesh(
        mesh.devices.reshape(4, 4, 2, mesh.shape["group"]), ("dp_0", "dp_1", "dp_2", "group")
    )
    return jax.shard_map(
        body,
        mesh=torus,
        in_specs=(P(DP, "group"), P(DP, "group"), P(), P(DP, "group")),
        out_specs=(P(DP, "group"), P("group")),
        check_vma=False,
    )
```

```python
import math

import jax
import jax.numpy as jnp
from jax import lax
from jax.experimental import pallas as pl
from jax.experimental.pallas import tpu as pltpu
from jax.sharding import Mesh
from jax.sharding import PartitionSpec as P

GW = 64
ITERS = 5
DP = ("dp_0", "dp_1", "dp_2")
EPSILON = 1e-05
CHUNKS = (26, 26)
f32, bf16 = jnp.float32, jnp.bfloat16
VMEM = pl.BlockSpec(memory_space=pltpu.VMEM)
HBM = pl.BlockSpec(memory_space=pltpu.HBM)


def shifted(value, axis, by):
    size = lax.axis_size(axis)
    return lax.ppermute(value, axis, [(i, (i + by) % size) for i in range(size)])


def gathered_weights(shard):
    count = lax.axis_size(DP)
    copies = jnp.broadcast_to(shard, (count, *shard.shape))
    parts = lax.all_to_all(copies, DP, split_axis=0, concat_axis=0, tiled=True)
    return parts.reshape(-1, shard.shape[1])


def after(value, *others):
    return lax.optimization_barrier((value, *others))


def half_of(block, lower):
    half = block.shape[0] // 2

    def kernel(ref, out):
        out[...] = ref[:half, :] if lower else ref[half:, :]

    return small_call(
        kernel, (jax.ShapeDtypeStruct((half, block.shape[1]), block.dtype),), (block,), "half_of"
    )[0]


def sums_over_ring(chunks, starts, cot, shard):
    weights = gathered_weights(shard)
    sides = [([c], [c]) for c in chunks]
    for hop in range(3):
        for index, (r, l) in enumerate(sides):
            if hop == 1 and index == 1:
                r[1], weights = after(r[1], weights)
            r.append(shifted(r[-1], "group", 1))
            l.append(shifted(l[-1], "group", -1))
    totals = None
    laid, fars = [], []
    for r, l in sides:
        if laid:
            big, near, sx = laid[0]
            r[3], l[3], sx = after(r[3], l[3], sx)
            laid[0] = (big, near, sx)
        fars.append(
            (shifted(half_of(r[3], True), "group", 1), shifted(half_of(l[3], False), "group", -1))
        )
        laid.append(near_step((*r, *l[1:]), weights))
    for (far_r, far_l), here, start in zip(fars, laid, starts):
        totals = far_step(far_r, far_l, here, cot, start, weights, totals)
    return totals


TILES = 2


def near_step(blocks, weights):
    width, tokens = blocks[0].shape
    channels = weights.shape[1]
    rows = 8 * width
    tile = tokens // TILES
    ahead = (0, 7, 6, 5, 1, 2, 3)

    def kernel(own, r1, r2, r3, l1, l2, l3, w, big, near, sx, sems):
        z = lax.axis_index("group")
        refs = (own, r1, r2, r3, l1, l2, l3)

        def place(by):
            return pl.ds(pl.multiple_of(((z + by) % 8) * width, 32), width)

        moves = [
            [
                pltpu.make_async_copy(
                    ref.at[:, step * tile : (step + 1) * tile],
                    big.at[step, place(by), :],
                    sems.at[step, index],
                )
                for index, (ref, by) in enumerate(zip(refs, ahead))
            ]
            for step in range(TILES)
        ]
        for step in moves:
            for move in step:
                move.start()
        for step in range(TILES):
            big[step, place(4), :] = jnp.zeros((width, tile), bf16)
            big[step, rows + channels :, :] = jnp.ones((16, tile), bf16)
        wt = w[...].astype(f32).T.astype(bf16)
        sx[place(4), :] = jnp.zeros((width, channels), f32)
        for ref, by in zip(refs, ahead):
            total = jnp.sum(ref[...].astype(f32), axis=1, keepdims=True)
            sx[place(by), :] = jnp.broadcast_to(total, (width, channels))
        for step in range(TILES):
            for move in moves[step]:
                move.wait()
            near[step] = jnp.dot(wt, big[step, :rows, :], preferred_element_type=f32)

    return pl.pallas_call(
        kernel,
        out_shape=(
            jax.ShapeDtypeStruct((TILES, rows + channels + 16, tile), bf16),
            jax.ShapeDtypeStruct((TILES, channels, tile), f32),
            jax.ShapeDtypeStruct((rows, channels), f32),
        ),
        in_specs=[VMEM] * 8,
        out_specs=(VMEM,) * 3,
        scratch_shapes=[pltpu.SemaphoreType.DMA((TILES, 7))],
        cost_estimate=pl.CostEstimate(
            flops=2 * tokens * rows * channels, bytes_accessed=2 * tokens * rows, transcendentals=0
        ),
        compiler_params=pltpu.CompilerParams(vmem_limit_bytes=14 * 1024 * 1024),
        name="near",
    )(*blocks, weights)


def far_step(far_r, far_l, laid, cot, start, weights, totals):
    half, tokens = far_r.shape
    width = 2 * half
    channels = cot.shape[1]
    rows = 8 * width
    tile = tokens // TILES
    accumulate = totals is not None

    def kernel(*refs):
        far_r, far_l, big_in, near, near_sx, cot, w = refs[:7]
        ins, rest = (refs[7:10], refs[10:]) if accumulate else ((), refs[7:])
        big, ab, hg, sx, ce, sems = rest
        row = pl.multiple_of(((lax.axis_index("group") + 4) % 8) * width, 32)

        moves = [
            [
                pltpu.make_async_copy(
                    far_r.at[:, step * tile : (step + 1) * tile],
                    big.at[step, pl.ds(row, half), :],
                    sems.at[step, 0],
                ),
                pltpu.make_async_copy(
                    far_l.at[:, step * tile : (step + 1) * tile],
                    big.at[step, pl.ds(pl.multiple_of(row + half, 16), half), :],
                    sems.at[step, 1],
                ),
                pltpu.make_async_copy(
                    cot.at[start + step * tile : start + (step + 1) * tile, :],
                    ce.at[step, :, :channels],
                    sems.at[step, 2],
                ),
            ]
            for step in range(TILES)
        ]
        for step in moves:
            for move in step:
                move.start()
        w_far = w[pl.ds(row, width), :].astype(f32).T.astype(bf16)
        far_sx = jnp.concatenate(
            [
                jnp.sum(ref[...].astype(f32), axis=1, keepdims=True)
                for ref in (far_r, far_l)
            ],
            axis=0,
        )
        sums = near_sx[...] + ins[2][...] if accumulate else near_sx[...]
        sx[...] = sums
        sx[pl.ds(row, width), :] = sx[pl.ds(row, width), :] + far_sx
        for step in moves:
            for move in step:
                move.wait()
        for step in range(TILES):
            et = near[step] + jnp.dot(
                w_far, big[step, pl.ds(row, width), :], preferred_element_type=f32
            )
            big[step, rows : rows + channels, :] = et.astype(bf16)
            ce[step, :, channels:] = et.T.astype(bf16)
            product = jnp.dot(big[step], ce[step], preferred_element_type=f32)
            if step or accumulate:
                before = (ab, hg) if step else ins
                ab[...] = before[0][...] + product[:rows]
                hg[...] = before[1][...] + product[rows : rows + channels + 8]
            else:
                ab[...] = product[:rows]
                hg[...] = product[rows : rows + channels + 8]

    aliases = {2: 0}
    if accumulate:
        aliases.update({7: 1, 8: 2, 9: 3})
    outs = pl.pallas_call(
        kernel,
        out_shape=(
            jax.ShapeDtypeStruct(laid[0].shape, bf16),
            jax.ShapeDtypeStruct((rows, 2 * channels), f32),
            jax.ShapeDtypeStruct((channels + 8, 2 * channels), f32),
            jax.ShapeDtypeStruct((rows, channels), f32),
        ),
        in_specs=[VMEM] * 5 + [HBM] + [VMEM] * (4 if accumulate else 1),
        out_specs=(VMEM,) * 4,
        scratch_shapes=[
            pltpu.VMEM((TILES, tile, 2 * channels), bf16),
            pltpu.SemaphoreType.DMA((TILES, 3)),
        ],
        input_output_aliases=aliases,
        cost_estimate=pl.CostEstimate(
            flops=2 * tokens * (rows + channels) * 2 * channels,
            bytes_accessed=2 * tokens * rows,
            transcendentals=0,
        ),
        compiler_params=pltpu.CompilerParams(vmem_limit_bytes=14 * 1024 * 1024),
        name="far",
    )(far_r, far_l, *laid, cot, weights, *(totals or ()))
    return outs[1:]


def small_call(kernel, outs, operands, name):
    return pl.pallas_call(
        kernel,
        out_shape=outs,
        in_specs=[VMEM] * len(operands),
        out_specs=tuple(VMEM for _ in outs),
        cost_estimate=pl.CostEstimate(flops=1_000_000, bytes_accessed=1_000_000, transcendentals=0),
        compiler_params=pltpu.CompilerParams(vmem_limit_bytes=6 * 1024 * 1024),
        name=name,
    )(*operands)


COMMON = 112
FAR_FIRST = (2, 1, 3)


def core_stage(totals):
    ab, hg, sx = totals
    share = 24
    channels = ab.shape[1] // 2

    def kernel(ab, hg, sx, keep, send):
        core = lax.axis_index("dp_2")
        for ref, parity in ((keep, core), (send, 1 - core)):
            for block in range(16):
                from_block = jnp.where(parity == 0, block, block % 4 * 4 + block // 4)
                row = pl.multiple_of((from_block * 2 + parity) * share, 8)
                for side in range(2):
                    to = (block * 2 + side) * share
                    ref[to : to + share, :] = ab[
                        pl.ds(row, share), side * channels : (side + 1) * channels
                    ]
            lane = lax.broadcasted_iota(jnp.int32, (GW, channels), 1)
            row = lax.broadcasted_iota(jnp.int32, (GW, channels), 0)
            low = lane < GW
            mixed, gram = (
                jnp.where(low, hg[:GW, cols], hg[GW : 2 * GW, cols])
                for cols in (slice(0, channels), slice(channels, 2 * channels))
            )
            base = 32 * share
            ref[base : base + GW, :] = mixed
            square = jnp.where(row < lane, gram, pltpu.roll(gram, GW, 1))
            ref[base + GW : base + GW + 32, :] = jnp.where(
                low[:32], square[:32], pltpu.roll(square, GW, 1)[32:]
            )
            base += GW + 32
            ref[base : base + 16, :] = jnp.zeros((16, channels), f32)
            diagonal = (lane == row) | (lane == row + GW)
            square_eye = lax.broadcasted_iota(
                jnp.int32, (channels, channels), 0
            ) == lax.broadcasted_iota(jnp.int32, (channels, channels), 1)
            ref[base : base + 1, :] = jnp.sum(
                jnp.where(diagonal, gram, 0.0), axis=0, keepdims=True
            )
            for side in range(2):
                ref[base + 1 + side : base + 2 + side, :] = hg[
                    2 * GW : 2 * GW + 1, side * channels : (side + 1) * channels
                ]
            for part in range(6):
                ref[base + 3 + part : base + 4 + part, :] = jnp.sum(
                    jnp.where(square_eye, sx[part * channels : (part + 1) * channels, :], 0.0),
                    axis=0,
                    keepdims=True,
                )

    shape = jax.ShapeDtypeStruct((32 * share + COMMON, channels), f32)
    return small_call(kernel, (shape, shape), (ab, hg, sx), "core_stage")


def axis_stage(first, received, rows_out):
    rows_in, channels = received[0].shape

    def kernel(*refs):
        ins, outs = refs[: len(received)], refs[len(received) :]
        core_zero = lax.axis_index("dp_2") == 0
        here = jnp.where(
            core_zero if first else ~core_zero, lax.axis_index("dp_0"), lax.axis_index("dp_1")
        )
        shared = ins[0][rows_in - COMMON :, :]
        for ref in ins[1:]:
            shared = shared + ref[rows_in - COMMON :, :]
        for step, out in enumerate(outs):
            row = pl.multiple_of(((here + step) % 4) * rows_out, 8)
            block = ins[0][pl.ds(row, rows_out), :]
            for ref in ins[1:]:
                block = block + ref[pl.ds(row, rows_out), :]
            out[:rows_out, :] = block
            out[rows_out:, :] = shared

    shape = jax.ShapeDtypeStruct((rows_out + COMMON, channels), f32)
    return small_call(kernel, (shape,) * 4, received, "axis_stage")


def crossed(value, first, by):
    pairs = []
    for y in range(4):
        for x in range(4):
            for core in range(2):
                along_y = (core == 0) == first
                to = ((y + by) % 4, x) if along_y else (y, (x + by) % 4)
                pairs.append(((y * 4 + x) * 2 + core, (to[0] * 4 + to[1]) * 2 + core))
    return lax.ppermute(value, DP, pairs)


def split(value):
    high = value.astype(bf16)
    return high, (value - high.astype(f32)).astype(bf16)


def dot(left, right):
    left_high, left_low = split(left)
    right_high, right_low = split(right)
    both = jnp.concatenate([left_high, left_low], axis=1)
    twice = jnp.concatenate([right_high, right_high], axis=0)
    return jnp.dot(both, twice, preferred_element_type=f32) + jnp.dot(
        left_high, right_low, preferred_element_type=f32
    )


def last_stage(received, gain, total_tokens):
    channels = received[0].shape[1]
    share = 24
    loss_scale = 1.0 / math.sqrt(total_tokens)
    inverse = 1.0 / total_tokens

    def kernel(*refs):
        ins, gain_ref = refs[: len(received)], refs[len(received)]
        weight_out, gain_out = refs[len(received) + 1 :]
        everything = ins[0][...]
        for ref in ins[1:]:
            everything = everything + ref[...]
        a_rows = everything[:share]
        b_rows = everything[share : 2 * share]
        base = 2 * share
        lane = lax.broadcasted_iota(jnp.int32, (channels, channels), 1)
        row = lax.broadcasted_iota(jnp.int32, (channels, channels), 0)
        same = (lane < GW) == (row < GW)
        eye = (lane == row).astype(f32)
        lane1 = lax.broadcasted_iota(jnp.int32, (1, channels), 1)

        def blocks(flat):
            return jnp.where(same, jnp.concatenate([flat, flat], axis=0), 0.0)

        def per_group(line):
            low = jnp.sum(jnp.where(lane1 < GW, line, 0.0), axis=1, keepdims=True)
            high = jnp.sum(jnp.where(lane1 < GW, 0.0, line), axis=1, keepdims=True)
            return jnp.where(lane1 < GW, low, high)

        def column(line):
            return jnp.sum(eye * line, axis=1, keepdims=True)

        h_t = blocks(everything[base : base + GW])
        packed = everything[base + GW : base + GW + 32]
        square = jnp.concatenate([packed, pltpu.roll(packed, GW, 1)], axis=0)
        square = jnp.where(lane[:GW] < GW, square, 0.0)
        square = jnp.concatenate([square, jnp.zeros((GW, channels), f32)], axis=0)
        turned = square.T
        upper = jnp.where(row < lane, square, turned)
        lower = jnp.where(row > lane, square, turned)
        lower = pltpu.roll(jnp.concatenate([lower[GW:], lower[:GW]], axis=0), GW, 1)
        base += GW + 32
        gram = jnp.where(row < GW, upper, lower)
        gram = jnp.where(same & (lane != row), gram, 0.0) + eye * everything[base : base + 1]
        cot_sum = everything[base + 1 : base + 2]
        mean = everything[base + 2 : base + 3] * inverse
        patch_sums = everything[base + 3 : base + 9]
        mean_col = column(mean)
        covariance = gram * inverse - jnp.where(same, mean_col * mean, 0.0) + EPSILON * eye
        h_t = h_t - jnp.where(same, mean_col * cot_sum, 0.0)
        scaled_gain = gain_ref[pl.ds(lax.axis_index("group"), 1), :] * loss_scale
        q_t = h_t * scaled_gain
        toward = 0.5 * (q_t + q_t.T)
        trace = per_group(jnp.sum(covariance * eye, axis=0, keepdims=True))
        normed = covariance / trace
        power = 1.5 * eye - 0.5 * normed
        change = -0.5 * toward
        right = jnp.concatenate([normed, toward], axis=1)
        for _ in range(ITERS - 1):
            both = jnp.concatenate([power, change], axis=0)
            first = dot(both, power)
            second = dot(both, right)
            square, mixed = first[:channels], first[channels:]
            times = second[:channels, :channels]
            times_change = second[channels:, :channels] + second[:channels, channels:]
            square_change = mixed + mixed.T
            third = dot(square, jnp.concatenate([times, times_change], axis=1))
            fourth = dot(square_change, times)
            power, change = (
                1.5 * power - 0.5 * third[:, :channels],
                1.5 * change - 0.5 * (third[:, channels:] + fourth),
            )
        root = lax.rsqrt(trace)
        whitener = power * root
        spread = per_group(jnp.sum(change * covariance, axis=0, keepdims=True))
        scale_part = per_group(jnp.sum(toward * power, axis=0, keepdims=True))
        cubed = root * root * root
        grad_cov = cubed * change - eye * (cubed * root * root * spread + 0.5 * cubed * scale_part)
        symmetric = grad_cov * (2.0 * inverse)
        gain_out[...] = jnp.sum(whitener * h_t, axis=0, keepdims=True) * loss_scale
        device = lax.axis_index(DP)
        lanes = lax.broadcasted_iota(jnp.int32, (share, channels), 1)
        rows = lax.broadcasted_iota(jnp.int32, (share, channels), 0) + device * share
        picked = jnp.zeros((share, channels), f32)
        for part in range(6):
            picked = picked + jnp.where(
                lanes + part * channels == rows, patch_sums[part : part + 1], 0.0
            )
        patch_sum = jnp.sum(picked, axis=1, keepdims=True)
        a_rows = (a_rows - patch_sum * (cot_sum * inverse)) * scaled_gain
        b_rows = b_rows - patch_sum * mean
        weight_out[...] = dot(a_rows, whitener) + dot(b_rows, symmetric)

    outs = (
        jax.ShapeDtypeStruct((share, channels), f32),
        jax.ShapeDtypeStruct((1, channels), f32),
    )
    return small_call(kernel, outs, (*received, gain), "last_stage")


def body(patches, embed_weight, channel_gain, cotangent):
    tok_rows = patches.shape[0]
    total_tokens = tok_rows * lax.axis_size(DP)
    unit = tok_rows // sum(CHUNKS)
    bounds = [unit * sum(CHUNKS[:i]) for i in range(len(CHUNKS) + 1)]
    flipped = patches.T
    totals = sums_over_ring(
        [flipped[:, lo:hi] for lo, hi in zip(bounds, bounds[1:])], bounds, cotangent, embed_weight
    )
    keep, send = core_stage(totals)
    keep, *send = axis_stage(True, (keep, shifted(send, "dp_2", 1)), 192)
    came = [crossed(send[by - 1], True, by) for by in FAR_FIRST]
    keep, *send = axis_stage(False, (keep, *came), 48)
    came = [crossed(send[by - 1], False, by) for by in FAR_FIRST]
    gain = channel_gain.reshape(-1, embed_weight.shape[1])
    weight_grad, gain_grad = last_stage((keep, *came), gain, total_tokens)
    return weight_grad, gain_grad.reshape(-1)


def solution(mesh):
    torus = Mesh(
        mesh.devices.reshape(4, 4, 2, mesh.shape["group"]), ("dp_0", "dp_1", "dp_2", "group")
    )
    return jax.shard_map(
        body,
        mesh=torus,
        in_specs=(P(DP, "group"), P(DP, "group"), P(), P(DP, "group")),
        out_specs=(P(DP, "group"), P("group")),
        check_vma=False,
    )
```
